32 devices in a mesh: inter: 16 (over z, y, core), intra: 2 (over x).
Axes of the slice: x: 2, y: 2, z: 4, core: 2. Of those that a mesh axis runs over, the one named last changes fastest.
Arguments:
- hidden_in: bfloat16 [16, 256, 4096], P('inter', 'intra'), may hold values from -120 to 120, as said below
- norm_gain: bfloat16 [4096], P(('inter', 'intra')), may hold values from 0.5 to 2, as said below
- qkv_weight: bfloat16 [4096, 768], P(('inter', 'intra')), may hold values from -0.09375 to 0.09375
- attn_cotangent: bfloat16 [16, 256, 512], P('inter', 'intra'), may hold values from -6 to 6
Outputs:
- attn: bfloat16 [16, 256, 512], P('inter', 'intra')
- grad_in: bfloat16 [16, 256, 4096], P('inter', 'intra')
- weight_grad: float32 [4096, 768], P(('intra', 'inter'))
- gain_grad: float32 [4096], P(('intra', 'inter'))
The draws below stay inside these ranges and needn't reach their ends.
Inputs may be any that keep to these rules, and one draw needn't show every extreme that they name: `hidden_in`: activations with spread row and feature scales. `norm_gain`: positive gains.
All inputs are finite; a program needn't handle non-finite values.
Results may differ from the reference program's by a relative error of at most 0.015.
Values may be sent and summed in bfloat16 or wider, within the bound.
No kernel may reach another device: no remote copies, remote signals or barrier semaphores. Data moves between devices by JAX's collectives and lax.ppermute only.
A program may use at most 64 MiB of HBM per device.

```python
import math
import jax
import jax.numpy as jnp
from jax import lax

D = 4096
HD = 128
HEADS = 4
SEQ = 256
SEQS = 16


def draw_hidden_in(key, part):
    key_base, key_rows, key_cols = jax.random.split(jax.random.fold_in(key, 11), 3)
    shape = (SEQS, SEQ, D)
    row_scale = jnp.exp(jax.random.uniform(key_rows, (SEQS, SEQ, 1), minval=0.0, maxval=math.log(10.0)))
    col_scale = jnp.exp(jax.random.uniform(key_cols, (1, 1, D), minval=math.log(0.5), maxval=math.log(3.0)))
    base = jnp.clip(jax.random.normal(key_base, shape), -4.0, 4.0)
    return (base * row_scale * col_scale).astype(jnp.bfloat16)


def draw_norm_gain(key, part):
    key_gain = jax.random.fold_in(key, 23)
    values_out = jnp.exp(jax.random.uniform(key_gain, (D,), minval=math.log(0.5), maxval=math.log(2.0)))
    return values_out.astype(jnp.bfloat16)


def block_scale(key, shape, cuts, least, high):
    loudness, own = 1.0, jax.random.fold_in(key, 6)
    for position, blocks in cuts:
        draws = jnp.exp(jax.random.uniform(jax.random.fold_in(own, position), (blocks,), jnp.float32, least / len(cuts), high / len(cuts)))
        loudness = loudness * jnp.repeat(draws, shape[position] // blocks).reshape([-1 if axis == position else 1 for axis in range(len(shape))])
    return loudness


def centred(stream_key, extent, width, bound, pieces=(), held_as=jnp.bfloat16):
    entries = width * jax.random.normal(stream_key, extent, jnp.float32)
    if pieces:
        entries = entries * block_scale(stream_key, extent, pieces, -0.22, 0.18)
    return jnp.clip(entries, -bound, bound).astype(held_as)


def setup_inputs(seed: int = 0) -> dict:
    arg_keys = jax.random.split(jax.random.key(seed), 5)
    return {
        "hidden_in": draw_hidden_in(jax.random.fold_in(arg_keys[4], 71), 0),
        "norm_gain": draw_norm_gain(jax.random.fold_in(arg_keys[4], 71), 0),
        "qkv_weight": centred(arg_keys[2], (D, (HEADS + 2) * HD), D ** -0.5, 0.09375, ((0, 32),)),
        "attn_cotangent": centred(arg_keys[3], (SEQS, SEQ, HEADS * HD), 1.0, 6.0, ((0, 16), (1, 2))),
    }


eps_norm = 1e-05
rope_base = 500000.0

def rope_tables(positions, head_size):
    half_size = head_size // 2
    freqs = rope_base ** (-jnp.arange(half_size, dtype=jnp.float32) / half_size)
    angles = positions.astype(jnp.float32)[:, None] * freqs[None, :]
    return (jnp.cos(angles), jnp.sin(angles))

def rotate(values_in, cosine, sine):
    half_size = values_in.shape[-1] // 2
    first, second = (values_in[..., :half_size], values_in[..., half_size:])
    return jnp.concatenate([first * cosine - second * sine, second * cosine + first * sine], axis=-1)

def unrotate(grad_out, cosine, sine):
    half_size = grad_out.shape[-1] // 2
    first, second = (grad_out[..., :half_size], grad_out[..., half_size:])
    return jnp.concatenate([first * cosine + second * sine, second * cosine - first * sine], axis=-1)

def reference(hidden_in, norm_gain, qkv_weight, attn_cotangent):
    gain = norm_gain.astype(jnp.float32)
    positions = jnp.arange(SEQ, dtype=jnp.int32)
    cosine, sine = rope_tables(positions, HD)
    row_pos = jnp.arange(SEQ * HEADS, dtype=jnp.int32) // HEADS
    allowed = positions[None, :] <= row_pos[:, None]
    scale = HD ** (-0.5)
    qcols = HEADS * HD

    def one_sequence(carry, items):
        weight_acc, gain_acc = carry
        rows_in, grad_attn = items
        wide_rows = rows_in.astype(jnp.float32)
        inv_rms = lax.rsqrt(lax.optimization_barrier(jnp.mean(wide_rows * wide_rows, axis=1, keepdims=True)) + eps_norm)
        normed = (wide_rows * inv_rms * gain[None, :]).astype(jnp.bfloat16)
        mixed = jnp.dot(normed, qkv_weight, preferred_element_type=jnp.float32)
        query = (rotate(mixed[:, :qcols].reshape(SEQ, HEADS, HD), cosine[:, None, :], sine[:, None, :]) * scale).astype(jnp.bfloat16).reshape(SEQ * HEADS, HD)
        key_rows = rotate(mixed[:, qcols:qcols + HD], cosine, sine).astype(jnp.bfloat16)
        value_rows = mixed[:, qcols + HD:].astype(jnp.bfloat16)
        grad_flat = grad_attn.reshape(SEQ * HEADS, HD)
        scores = jnp.dot(query, key_rows.T, preferred_element_type=jnp.float32)
        scores = jnp.where(allowed, scores, -1e+30)
        row_top = lax.optimization_barrier(jnp.max(scores, axis=1))
        row_total = lax.optimization_barrier(jnp.sum(jnp.where(allowed, jnp.exp(scores - row_top[:, None]), 0.0), axis=1))
        log_total = row_top + jnp.log(row_total)
        probs = jnp.where(allowed, jnp.exp(scores - log_total[:, None]), 0.0)
        probs_low = probs.astype(jnp.bfloat16)
        attn_flat = jnp.dot(probs, value_rows.astype(jnp.float32), precision=lax.Precision.HIGHEST, preferred_element_type=jnp.float32).astype(jnp.bfloat16)
        row_delta = lax.optimization_barrier(jnp.sum(grad_flat.astype(jnp.float32) * attn_flat.astype(jnp.float32), axis=1))
        grad_probs = jnp.dot(grad_flat, value_rows.T, preferred_element_type=jnp.float32)
        grad_scores = (probs * (grad_probs - row_delta[:, None])).astype(jnp.bfloat16)
        grad_query = jnp.dot(grad_scores, key_rows, preferred_element_type=jnp.float32)
        grad_keys = jnp.dot(grad_scores.T, query, preferred_element_type=jnp.float32)
        grad_values = jnp.dot(probs_low.T, grad_flat, preferred_element_type=jnp.float32)
        query_back = (unrotate(grad_query.reshape(SEQ, HEADS, HD), cosine[:, None, :], sine[:, None, :]) * scale).reshape(SEQ, qcols)
        grad_mixed = jnp.concatenate([query_back, unrotate(grad_keys, cosine, sine), grad_values], axis=1).astype(jnp.bfloat16)
        grad_normed = jnp.dot(grad_mixed, qkv_weight.T, preferred_element_type=jnp.float32)
        inner = lax.optimization_barrier(jnp.sum(grad_normed * gain[None, :] * wide_rows, axis=1, keepdims=True))
        grad_rows = (gain[None, :] * grad_normed * inv_rms - wide_rows * inv_rms ** 3 / D * inner).astype(jnp.bfloat16)
        gain_acc = gain_acc + lax.optimization_barrier(jnp.sum(grad_normed * wide_rows * inv_rms, axis=0))
        term_low = jnp.dot(normed.T, grad_mixed, preferred_element_type=jnp.float32).astype(jnp.bfloat16)
        term_low = lax.optimization_barrier(term_low)
        weight_acc = weight_acc + term_low.astype(jnp.float32)
        return ((weight_acc, gain_acc), (attn_flat.reshape(SEQ, qcols), grad_rows))
    start = (jnp.zeros((D, (HEADS + 2) * HD), jnp.float32), jnp.zeros((D,), jnp.float32))
    (weight_grad, gain_grad), (attn, grad_in) = lax.scan(one_sequence, start, (hidden_in, attn_cotangent))
    return (attn, grad_in, weight_grad, gain_grad)
```

```python
import jax
import jax.numpy as jnp
from jax import lax
from jax.experimental import pallas as pl
from jax.experimental.pallas import tpu as pltpu
from jax.sharding import PartitionSpec as P

HD = 128
HEADS = 4


eps_norm = 1e-05
rope_base = 500000.0


def rope_tables(positions, head_size):
    half_size = head_size // 2
    freqs = rope_base ** (-jnp.arange(half_size, dtype=jnp.float32) / half_size)
    angles = positions.astype(jnp.float32)[:, None] * freqs[None, :]
    return (jnp.cos(angles), jnp.sin(angles))


def rotate(values_in, cosine, sine):
    half_size = values_in.shape[-1] // 2
    first, second = (values_in[..., :half_size], values_in[..., half_size:])
    return jnp.concatenate(
        [first * cosine - second * sine, second * cosine + first * sine], axis=-1
    )


def unrotate(grad_out, cosine, sine):
    half_size = grad_out.shape[-1] // 2
    first, second = (grad_out[..., :half_size], grad_out[..., half_size:])
    return jnp.concatenate(
        [first * cosine + second * sine, second * cosine - first * sine], axis=-1
    )


def forward_fold(query_rows, row_pos):

    def forward_advance(carry, piece, start):
        row_top, row_total, weighted = carry
        key_part, value_part = piece
        scores = jnp.einsum("qd,kd->qk", query_rows, key_part, preferred_element_type=jnp.float32)
        key_pos = jnp.arange(key_part.shape[0], dtype=jnp.int32)
        allowed = key_pos[None, :] <= row_pos[:, None]
        scores = jnp.where(allowed, scores, -1e30)
        new_top = jnp.maximum(row_top, jnp.max(scores, axis=1))
        numbers = jnp.where(allowed, jnp.exp(scores - new_top[:, None]), 0.0)
        row_total = jnp.sum(numbers, axis=1)
        weighted = jnp.dot(
            numbers,
            value_part.astype(jnp.float32),
            precision=lax.Precision.HIGHEST,
            preferred_element_type=jnp.float32,
        )
        return (new_top, row_total, weighted)

    return forward_advance


def query_grad_fold(query_rows, row_pos, grad_flat, log_total, row_delta):

    def query_advance(grad_query, piece, start):
        key_part, value_part = piece
        scores = jnp.einsum("qd,kd->qk", query_rows, key_part, preferred_element_type=jnp.float32)
        key_pos = jnp.arange(key_part.shape[0], dtype=jnp.int32)
        allowed = key_pos[None, :] <= row_pos[:, None]
        probs = jnp.where(
            allowed, jnp.exp(jnp.where(allowed, scores, -1e30) - log_total[:, None]), 0.0
        )
        grad_probs = jnp.einsum(
            "qd,kd->qk", grad_flat, value_part, preferred_element_type=jnp.float32
        )
        grad_scores = (probs * (grad_probs - row_delta[:, None])).astype(jnp.bfloat16)
        return jnp.dot(grad_scores, key_part, preferred_element_type=jnp.float32)

    return query_advance


def key_grad_fold(key_rows, value_rows, key_pos, log_all, delta_all, heads_count):

    def key_advance(carry, piece, start):
        query_part, attn_grad_part = piece
        count = query_part.shape[0]
        scores = jnp.einsum("qd,kd->qk", query_part, key_rows, preferred_element_type=jnp.float32)
        query_pos = jnp.arange(count, dtype=jnp.int32) // heads_count
        allowed = key_pos[None, :] <= query_pos[:, None]
        probs = jnp.where(
            allowed, jnp.exp(jnp.where(allowed, scores, -1e30) - log_all[:, None]), 0.0
        )
        grad_values = jnp.einsum(
            "qk,qd->kd",
            probs.astype(jnp.bfloat16),
            attn_grad_part,
            preferred_element_type=jnp.float32,
        )
        grad_probs = jnp.einsum(
            "qd,kd->qk", attn_grad_part, value_rows, preferred_element_type=jnp.float32
        )
        grad_scores = (probs * (grad_probs - delta_all[:, None])).astype(jnp.bfloat16)
        grad_keys = jnp.einsum(
            "qk,qd->kd", grad_scores, query_part, preferred_element_type=jnp.float32
        )
        return (grad_keys, grad_values)

    return key_advance


def generic_local(hidden_in, norm_gain, qkv_weight, attn_cotangent):
    rows_in = hidden_in[0]
    grad_attn = attn_cotangent[0]
    tokens_here = rows_in.shape[0]
    width = rows_in.shape[1]
    head_size = HD
    heads_count = HEADS
    qcols = heads_count * head_size
    scale = head_size ** (-0.5)
    weight_group, gain_group = (
        lax.all_gather(qkv_weight, "intra", axis=0, tiled=True),
        lax.all_gather(norm_gain, "intra", axis=0, tiled=True),
    )
    weight_full, gain_full = (
        lax.all_gather(weight_group, "inter", axis=0, tiled=True),
        lax.all_gather(gain_group, "inter", axis=0, tiled=True),
    )
    query_pos = lax.axis_index("intra") * tokens_here + jnp.arange(tokens_here, dtype=jnp.int32)
    row_pos = jnp.broadcast_to(query_pos[:, None], (tokens_here, heads_count)).reshape(
        tokens_here * heads_count
    )
    cosine, sine = rope_tables(query_pos, head_size)
    wide_rows = rows_in.astype(jnp.float32)
    inv_rms = lax.rsqrt(jnp.mean(wide_rows * wide_rows, axis=1, keepdims=True) + eps_norm)
    normed = (wide_rows * inv_rms * gain_full.astype(jnp.float32)[None, :]).astype(jnp.bfloat16)
    mixed = jnp.dot(normed, weight_full, preferred_element_type=jnp.float32)
    query_rows = (
        (
            rotate(
                mixed[:, :qcols].reshape(tokens_here, heads_count, head_size),
                cosine[:, None, :],
                sine[:, None, :],
            )
            * scale
        )
        .astype(jnp.bfloat16)
        .reshape(tokens_here * heads_count, head_size)
    )
    key_rows = rotate(mixed[:, qcols : qcols + head_size], cosine, sine).astype(jnp.bfloat16)
    value_rows = mixed[:, qcols + head_size :].astype(jnp.bfloat16)
    grad_flat = grad_attn.reshape(tokens_here * heads_count, head_size)
    flat_rows = tokens_here * heads_count
    forward_step = forward_fold(query_rows, row_pos)
    start_carry = (
        jnp.full((flat_rows,), -1e30, jnp.float32),
        jnp.zeros((flat_rows,), jnp.float32),
        jnp.zeros((flat_rows, head_size), jnp.float32),
    )
    row_top, row_total, weighted = forward_step(
        start_carry,
        (
            lax.all_gather(key_rows, "intra", axis=0, tiled=True),
            lax.all_gather(value_rows, "intra", axis=0, tiled=True),
        ),
        jnp.int32(0),
    )
    attn_flat = (weighted / row_total[:, None]).astype(jnp.bfloat16)
    log_total = row_top + jnp.log(row_total)
    row_delta = jnp.sum(grad_flat.astype(jnp.float32) * attn_flat.astype(jnp.float32), axis=1)
    query_step = query_grad_fold(query_rows, row_pos, grad_flat, log_total, row_delta)
    grad_query = query_step(
        jnp.zeros((flat_rows, head_size), jnp.float32),
        (
            lax.all_gather(key_rows, "intra", axis=0, tiled=True),
            lax.all_gather(value_rows, "intra", axis=0, tiled=True),
        ),
        jnp.int32(0),
    )
    log_all, delta_all = (
        lax.all_gather(log_total, "intra", axis=0, tiled=True),
        lax.all_gather(row_delta, "intra", axis=0, tiled=True),
    )
    key_step = key_grad_fold(key_rows, value_rows, query_pos, log_all, delta_all, heads_count)
    grad_keys, grad_values = key_step(
        (
            jnp.zeros((tokens_here, head_size), jnp.float32),
            jnp.zeros((tokens_here, head_size), jnp.float32),
        ),
        (
            lax.all_gather(query_rows, "intra", axis=0, tiled=True),
            lax.all_gather(grad_flat, "intra", axis=0, tiled=True),
        ),
        jnp.int32(0),
    )
    query_back = (
        unrotate(
            grad_query.reshape(tokens_here, heads_count, head_size),
            cosine[:, None, :],
            sine[:, None, :],
        )
        * scale
    ).reshape(tokens_here, qcols)
    grad_mixed = jnp.concatenate(
        [query_back, unrotate(grad_keys, cosine, sine), grad_values], axis=1
    ).astype(jnp.bfloat16)
    weight_back, gain_back = (weight_full, gain_full)
    gain_wide = gain_back.astype(jnp.float32)[None, :]
    grad_normed = jnp.einsum(
        "tc,dc->td", grad_mixed, weight_back, preferred_element_type=jnp.float32
    )
    inner = jnp.sum(grad_normed * gain_wide * wide_rows, axis=1, keepdims=True)
    grad_rows = (
        gain_wide * grad_normed * inv_rms - wide_rows * inv_rms**3 / width * inner
    ).astype(jnp.bfloat16)
    gain_term = jnp.sum(grad_normed * wide_rows * inv_rms, axis=0)
    normed_cols = lax.all_to_all(normed, "intra", split_axis=1, concat_axis=0, tiled=True)
    group_term = lax.dot_general(
        normed_cols,
        lax.all_gather(grad_mixed, "intra", axis=0, tiled=True),
        (((0,), (0,)), ((), ())),
        preferred_element_type=jnp.float32,
    )
    term_low = lax.optimization_barrier(group_term.astype(jnp.bfloat16))
    gain_sums = lax.psum_scatter(gain_term, "intra", scatter_dimension=0, tiled=True)
    weight_grad, gain_grad = (
        lax.psum_scatter(term_low.astype(jnp.float32), "inter", scatter_dimension=0, tiled=True),
        lax.psum_scatter(gain_sums, "inter", scatter_dimension=0, tiled=True),
    )
    return (attn_flat.reshape(tokens_here, qcols)[None], grad_rows[None], weight_grad, gain_grad)


LANES = 128
NEG = -1e30


def partial_kernel(slots, own_ref, peer_ref, *rest):
    pieces, (out_ref, rows, sems) = rest[:-3], rest[-3:]
    block = pieces[0].shape[0]
    copies = [
        pltpu.make_async_copy(
            piece, rows.at[pl.ds(pl.multiple_of(slots[n] * block, block), block)], sems.at[n]
        )
        for n, piece in enumerate(pieces)
    ]
    for copy in copies:
        copy.start()
    for copy in copies:
        copy.wait()
    tokens = own_ref.shape[0]
    out_ref[:tokens] = jnp.dot(
        own_ref[...], rows[...], preferred_element_type=jnp.float32
    ).astype(jnp.bfloat16)
    out_ref[tokens:] = jnp.dot(
        peer_ref[...], rows[...], preferred_element_type=jnp.float32
    ).astype(jnp.bfloat16)


def back_kernel(slots, grads_ref, *rest):
    pieces, (own_ref, peer_ref, rows, sems) = rest[:-4], rest[-4:]
    block = pieces[0].shape[0]
    copies = [
        pltpu.make_async_copy(
            piece, rows.at[pl.ds(pl.multiple_of(slots[n] * block, block), block)], sems.at[n]
        )
        for n, piece in enumerate(pieces)
    ]
    for copy in copies:
        copy.start()
    for copy in copies:
        copy.wait()
    tokens = own_ref.shape[0]
    dims = (((1,), (1,)), ((), ()))
    peer_ref[...] = lax.dot_general(
        grads_ref[tokens:], rows[...], dims, preferred_element_type=jnp.float32
    ).astype(jnp.bfloat16)
    own_ref[...] = lax.dot_general(
        grads_ref[:tokens], rows[...], dims, preferred_element_type=jnp.float32
    )


def split_kernel(where, x_ref, own_ref, send_ref, own_half, send_half, rms_ref):
    j = where[0]
    tokens, width = x_ref.shape
    half = width // 2
    square = jnp.zeros((tokens, LANES), jnp.float32)
    for n in range(half // LANES):
        for part, out in ((j, own_ref), (1 - j, send_ref)):
            start = pl.multiple_of((2 * n + part) * LANES, LANES)
            piece = x_ref[:, pl.ds(start, LANES)]
            out[:, n * LANES : (n + 1) * LANES] = piece
            wide = piece.astype(jnp.float32)
            square = square + wide * wide
    own_half[...] = x_ref[:, pl.ds(pl.multiple_of(j * half, LANES), half)]
    send_half[...] = x_ref[:, pl.ds(pl.multiple_of((1 - j) * half, LANES), half)]
    total = jnp.sum(square, axis=1, keepdims=True)
    rms_ref[...] = jnp.broadcast_to(lax.rsqrt(total / width + eps_norm), (tokens, LANES))


def attention_kernel(
    where, part_ref, peer_ref, rms_own, rms_peer, cot_own, cot_peer, cos_ref, sin_ref,
    attn_ref, grads_ref, pull_ref, *, width,
):
    j = where[0]
    tokens = rms_own.shape[0]
    total = 2 * tokens
    qcols = HEADS * HD
    scale = HD ** (-0.5)
    swap = peer_ref[...].astype(jnp.float32)
    raw = part_ref[...].astype(jnp.float32) + jnp.concatenate([swap[tokens:], swap[:tokens]], axis=0)
    rms = jnp.concatenate([rms_own[...], rms_peer[...]], axis=0)
    rms_col = rms[:, :1]
    mixed = raw * rms_col
    cosine, sine = cos_ref[...], sin_ref[...]

    def turn(u):
        return u * cosine + pltpu.roll(u, HD // 2, 1) * sine

    def unturn(u):
        return u * cosine - pltpu.roll(u, HD // 2, 1) * sine

    def position(axis):
        index = lax.broadcasted_iota(jnp.int32, (total, total), axis)
        return jnp.where(index < tokens, index + j * tokens, index - j * tokens)

    allowed = position(1) <= position(0)
    keys = turn(mixed[:, qcols : qcols + HD]).astype(jnp.bfloat16)
    values = mixed[:, qcols + HD :].astype(jnp.bfloat16)
    grad_keys = jnp.zeros((total, HD), jnp.float32)
    grad_values = jnp.zeros((total, HD), jnp.float32)
    inner = jnp.zeros((total, HD), jnp.float32)
    rows_rows = (((1,), (1,)), ((), ()))
    cols_cols = (((0,), (0,)), ((), ()))

    def dot(a, b, dims):
        return lax.dot_general(a, b, dims, preferred_element_type=jnp.float32)

    for h in range(HEADS):
        span = slice(h * HD, (h + 1) * HD)
        query = (turn(mixed[:, span]) * scale).astype(jnp.bfloat16)
        cot = jnp.concatenate([cot_own[:, span], cot_peer[:, span]], axis=0)
        scores = jnp.where(allowed, dot(query, keys, rows_rows), NEG)
        top = jnp.max(scores, axis=1, keepdims=True)
        numbers = jnp.exp(scores - top)
        share = 1.0 / jnp.sum(numbers, axis=1, keepdims=True)
        probs = numbers * share
        probs_low = probs.astype(jnp.bfloat16)
        grad_probs = dot(cot, values, rows_rows)
        delta = jnp.sum(probs * grad_probs, axis=1, keepdims=True)
        grad_scores = (probs * (grad_probs - delta)).astype(jnp.bfloat16)
        attn_ref[:, span] = (
            jnp.dot(
                numbers[:tokens].astype(jnp.bfloat16), values, preferred_element_type=jnp.float32
            )
            * share[:tokens]
        ).astype(jnp.bfloat16)
        grad_query = unturn(jnp.dot(grad_scores, keys, preferred_element_type=jnp.float32)) * scale
        grads_ref[:, span] = (grad_query * rms_col).astype(jnp.bfloat16)
        inner = inner + grad_query * mixed[:, span]
        grad_keys = grad_keys + dot(grad_scores, query, cols_cols)
        grad_values = grad_values + dot(probs_low, cot, cols_cols)
    grad_keys = unturn(grad_keys)
    inner = inner + grad_keys * mixed[:, qcols : qcols + HD] + grad_values * mixed[:, qcols + HD :]
    grads_ref[:, qcols : qcols + HD] = (grad_keys * rms_col).astype(jnp.bfloat16)
    grads_ref[:, qcols + HD :] = (grad_values * rms_col).astype(jnp.bfloat16)
    pull = jnp.sum(inner[:tokens], axis=1, keepdims=True) * (1.0 / width)
    pull_ref[...] = pull * rms_own[...] * rms_own[...]


def term_kernel(slots, grads_ref, next_ref, a_ref, b_ref, c_ref, d_ref, *outs):
    tokens = a_ref.shape[0]
    dims = (((0,), (0,)), ((), ()))
    for n, out in enumerate(outs):
        block = out.shape[0]
        span = pl.ds(pl.multiple_of(slots[n] * block, block), block)
        cols = jnp.concatenate([a_ref[:, span], b_ref[:, span], c_ref[:, span], d_ref[:, span]], axis=0)
        rows = jnp.concatenate([grads_ref[...], next_ref[...]], axis=0)
        out[...] = lax.dot_general(
            cols, rows, dims, preferred_element_type=jnp.float32
        ).astype(jnp.bfloat16)


def grad_in_kernel(where, x_ref, own_ref, peer_ref, pull_ref, out_ref):
    j = where[0]
    pull = pull_ref[...]
    for n in range(x_ref.shape[1] // (2 * LANES)):
        cols = slice(n * LANES, (n + 1) * LANES)
        for part, src in ((j, own_ref), (1 - j, peer_ref)):
            span = pl.ds(pl.multiple_of((2 * n + part) * LANES, LANES), LANES)
            wide = x_ref[:, span].astype(jnp.float32)
            out_ref[:, span] = (src[:, cols].astype(jnp.float32) - wide * pull).astype(jnp.bfloat16)


def last_kernel(keep_ref, first_ref, *rest):
    others, (rows_ref, gain_ref, weight_out, gain_out) = rest[:-4], rest[-4:]
    total = keep_ref[...].astype(jnp.float32) + first_ref[...].astype(jnp.float32)
    for other in others:
        total = total + other[...].astype(jnp.float32)
    weight_out[...] = total * gain_ref[:, :1]
    gain_sum = jnp.sum(total * rows_ref[...].astype(jnp.float32), axis=1, keepdims=True)
    gain_out[...] = jnp.broadcast_to(gain_sum, gain_out.shape)


def call(kernel, out_shape, scalars, arrays, hbm=0, scratch=()):
    vmem = pl.BlockSpec(memory_space=pltpu.VMEM)
    anywhere = pl.BlockSpec(memory_space=pl.ANY)
    smem = pl.BlockSpec(memory_space=pltpu.SMEM)
    many = isinstance(out_shape, (tuple, list))
    specs = [smem] * len(scalars) + [vmem] * (len(arrays) - hbm) + [anywhere] * hbm
    return pl.pallas_call(
        kernel,
        out_shape=out_shape,
        in_specs=specs,
        out_specs=tuple(vmem for _ in out_shape) if many else vmem,
        scratch_shapes=scratch,
        compiler_params=pltpu.CompilerParams(vmem_limit_bytes=48 * 1024 * 1024),
    )(*scalars, *arrays)


def pair_local(groups, hidden_in, norm_gain, qkv_weight, attn_cotangent):
    depth = groups // 4
    rows_in, cot = hidden_in[0], attn_cotangent[0]
    tokens, width = rows_in.shape
    block, columns = qkv_weight.shape
    half = width // 2
    qcols = HEADS * HD
    i, j = lax.axis_index("inter"), lax.axis_index("intra")
    deep, side, core = i // 4, (i // 2) % 2, i % 2
    where = j.astype(jnp.int32)[None]
    low, full = jnp.bfloat16, jnp.float32

    def swap_pair(u):
        return lax.ppermute(u, "intra", [(0, 1), (1, 0)])

    def swap_core(u):
        return lax.ppermute(u, "inter", [(n, n ^ 1) for n in range(groups)])

    def swap_side(u):
        return lax.ppermute(u, "inter", [(n, n ^ 2) for n in range(groups)])

    def shift_deep(u, k):
        return lax.ppermute(u, "inter", [(n, (n + 4 * k) % groups) for n in range(groups)])

    def sds(shape, dtype):
        return jax.ShapeDtypeStruct(shape, dtype)

    def slot(k, l, m):
        return (((deep - k) % depth) * 4 + (side ^ l) * 2 + (core ^ m)).astype(jnp.int32)

    gain_col = norm_gain.astype(full)[:, None]
    weight_rows = (qkv_weight.astype(full) * gain_col).astype(low)
    by_deep = [weight_rows] + [shift_deep(weight_rows, k) for k in range(1, depth)]
    by_side = [swap_side(u) for u in by_deep]
    pieces, slots = [], []
    for l, group in enumerate((by_deep, by_side)):
        for k, u in enumerate(group):
            pieces += [u, swap_core(u)]
            slots += [slot(k, l, 0), slot(k, l, 1)]
    slots = jnp.stack(slots)

    x_own, x_send, half_own, half_send, rms = call(
        split_kernel,
        (
            sds((tokens, half), low),
            sds((tokens, half), low),
            sds((tokens, half), low),
            sds((tokens, half), low),
            sds((tokens, LANES), full),
        ),
        (where,),
        (rows_in,),
    )
    x_peer = swap_pair(x_send)
    rms_peer = swap_pair(rms)
    cot_peer = swap_pair(cot)
    half_peer = swap_pair(half_send)

    copies = [pltpu.VMEM((half, columns), low), pltpu.SemaphoreType.DMA((len(pieces),))]
    part = call(
        partial_kernel,
        sds((2 * tokens, columns), low),
        (slots,),
        (x_own, x_peer, *pieces),
        hbm=len(pieces),
        scratch=copies,
    )
    part_peer = swap_pair(part)

    local_pos = jnp.arange(tokens, dtype=jnp.int32)
    positions = jnp.concatenate([j * tokens + local_pos, (1 - j) * tokens + local_pos])
    cosine, sine = rope_tables(positions, HD)
    cos_full = jnp.concatenate([cosine, cosine], axis=1)
    sin_full = jnp.concatenate([-sine, sine], axis=1)

    attn, grads, pull = call(
        lambda *refs: attention_kernel(*refs, width=width),
        (sds((tokens, qcols), low), sds((2 * tokens, columns), low), sds((tokens, LANES), full)),
        (where,),
        (part, part_peer, rms, rms_peer, cot, cot_peer, cos_full, sin_full),
    )

    grads_next = swap_core(grads)
    own_next, peer_next = swap_core(half_own), swap_core(half_peer)

    order = [k for k in range(depth) if k] + [0]
    picks = jnp.stack(
        [
            ((((deep + k) % depth) * 2 + (side ^ l)) * 2 + core).astype(jnp.int32)
            for l in (1, 0)
            for k in order
        ]
    )
    terms = call(
        term_kernel,
        tuple(sds((block, columns), low) for _ in range(2 * depth)),
        (picks,),
        (grads, grads_next, half_own, half_peer, own_next, peer_next),
    )
    arrived = [swap_side(u) for u in terms[:depth]]
    kept = terms[depth:]
    others = []
    for n, k in enumerate(order[:-1]):
        merged = (arrived[n].astype(full) + kept[n].astype(full)).astype(low)
        others.append(shift_deep(merged, k))

    y_own, y_send = call(
        back_kernel,
        (sds((tokens, half), full), sds((tokens, half), low)),
        (slots,),
        (grads, *pieces),
        hbm=len(pieces),
        scratch=copies,
    )
    y_peer = swap_pair(y_send)
    grad_in = call(
        grad_in_kernel,
        sds((tokens, width), low),
        (where,),
        (rows_in, y_own, y_peer, pull),
    )

    moves = [(n, (n % groups) * 2 + n // groups) for n in range(2 * groups)]
    rows_out = lax.ppermute(qkv_weight, ("inter", "intra"), moves)
    gain_out = lax.ppermute(norm_gain, ("inter", "intra"), moves)
    weight_grad, gain_wide = call(
        last_kernel,
        (sds((block, columns), full), sds((block, LANES), full)),
        (),
        (
            kept[-1],
            arrived[-1],
            *others,
            rows_out,
            jnp.broadcast_to(gain_out.astype(full)[:, None], (block, LANES)),
        ),
    )
    return (attn[None], grad_in[None], weight_grad, gain_wide[:, 0])


def solution(mesh):
    groups, pair = mesh.shape["inter"], mesh.shape["intra"]

    def local(hidden_in, norm_gain, qkv_weight, attn_cotangent):
        fits = pair == 2 and groups % 4 == 0 and qkv_weight.shape[0] % LANES == 0
        args = (hidden_in, norm_gain, qkv_weight, attn_cotangent)
        return pair_local(groups, *args) if fits else generic_local(*args)

    return jax.shard_map(
        local,
        mesh=mesh,
        in_specs=(
            P("inter", "intra", None),
            P(("inter", "intra")),
            P(("inter", "intra"), None),
            P("inter", "intra", None),
        ),
        out_specs=(
            P("inter", "intra", None),
            P("inter", "intra", None),
            P(("intra", "inter"), None),
            P(("intra", "inter")),
        ),
        check_vma=False,
    )
```
